32 devices in a mesh: rows: 8 (over z, y), par: 4 (over x, core).
Axes of the slice: x: 2, y: 2, z: 4, core: 2. Of those that a mesh axis runs over, the one named last changes fastest.
Arguments:
- base_a: bfloat16 [4, 64, 256], P(None, 'rows'), may hold values from -6 to 6
- base_b: bfloat16 [4, 64, 256], P(None, 'rows'), may hold values from -6 to 6
- input_scale: float32 [256], replicated, may hold values from 0.1 to 3
- layer_one: bfloat16 [256, 1024], replicated, may hold values from -0.375 to 0.375
- layer_two: bfloat16 [1024, 1024], replicated, may hold values from -0.1875 to 0.1875
- layer_three: bfloat16 [1024, 128], replicated, may hold values from -0.1875 to 0.1875
- swap_cols: int32 [256], P('par'), may hold values from 0 to 255, each once
- window_ends: int32 [4], replicated, may hold values from 32 to 64
Outputs:
- first_order: float32 [4, 256, 128], P(None, 'par')
- total_order: float32 [4, 256, 128], P(None, 'par')
- total_variance: float32 [4, 128], replicated
The draws below stay inside these ranges and needn't reach their ends.
Inputs may be any that keep to these rules, and one draw needn't show every extreme that they name: window w uses its rows 0 to window_ends[w] - 1. `swap_cols`: each column appears once.
All inputs are finite; a program needn't handle non-finite values.
Results may differ from the reference program's by a relative error of at most 0.0055.
The reference program's roundings to bfloat16 on the way (of `inputs_a`, `inputs_b`, `inputs_c`, `hidden_one` and `hidden_two`) count: a program that leaves them out, or rounds other values in their place, can miss the bound.
Values sent between devices are 32-bit elements; how exact they have to be, the bound alone decides.
No kernel may reach another device: no remote copies, remote signals or barrier semaphores. Data moves between devices by JAX's collectives and lax.ppermute only.
A program may use at most 64 MiB of HBM per device.

```python
import math
import jax
import jax.numpy as jnp
from jax import lax

D = 256
HIDDEN_SIZE = 1024
OUTPUTS = 128
WINDOWS = 4
WINDOW_ROWS = 64


def place_ends(values, key, least, top_value):
    longest = values.shape.index(max(values.shape))
    spots = []
    for shift in (0, 1):
        where = [jax.random.randint(jax.random.fold_in(key, axis), (), 0, length) for axis, length in enumerate(values.shape)]
        where[longest] = (where[longest] + shift) % values.shape[longest]
        spots.append(tuple(where))
    return values.at[spots[0]].set(least).at[spots[1]].set(top_value)


def block_scale(stream_key, extent, split, low, largest):
    def one(axis_at, shards_of):
        steps = jax.random.uniform(jax.random.fold_in(jax.random.fold_in(stream_key, 6), axis_at), (shards_of,), jnp.float32, low / len(split), largest / len(split))
        return jnp.repeat(jnp.exp(steps), extent[axis_at] // shards_of).reshape((-1,) + (1,) * (len(extent) - axis_at - 1))

    level = one(*split[0])
    for cut in split[1:]:
        level = level * one(*cut)
    return level


def noise(key, extent, spread, reach, split=(), held_as=jnp.bfloat16):
    entries = jax.random.normal(key, extent, jnp.float32) * spread
    if len(split) > 0:
        entries = block_scale(key, extent, split, -0.22, 0.18) * entries
    return jnp.clip(entries, min=-reach, max=reach).astype(held_as)


def setup_inputs(seed: int = 0) -> dict:
    key_of = jax.random.split(jax.random.key(seed), 9)
    base_a = noise(key_of[0], (WINDOWS, WINDOW_ROWS, D), 1.0, 6.0, ((1, 8),))
    base_b = noise(key_of[1], (WINDOWS, WINDOW_ROWS, D), 1.0, 6.0, ((1, 8),))
    input_scale = jnp.clip(jnp.exp(jax.random.uniform(key_of[2], (D,), jnp.float32, math.log(0.1), math.log(3.0))), 0.1, 3.0)
    layer_one = noise(key_of[3], (D, HIDDEN_SIZE), D ** -0.5, 0.375)
    layer_two = noise(key_of[4], (HIDDEN_SIZE, HIDDEN_SIZE), HIDDEN_SIZE ** -0.5, 0.1875)
    layer_three = noise(key_of[5], (HIDDEN_SIZE, OUTPUTS), HIDDEN_SIZE ** -0.5, 0.1875)
    swap_cols = jax.random.permutation(key_of[6], D).astype(jnp.int32)
    window_ends = place_ends(jax.random.randint(key_of[7], (WINDOWS,), WINDOW_ROWS // 2, WINDOW_ROWS + 1), jax.random.fold_in(key_of[7], 1), WINDOW_ROWS // 2, WINDOW_ROWS).astype(jnp.int32)
    return {"base_a": base_a, "base_b": base_b, "input_scale": input_scale, "layer_one": layer_one, "layer_two": layer_two, "layer_three": layer_three, "swap_cols": swap_cols, "window_ends": window_ends}


def network_tail(first_pre, layer_two, layer_three):
    hidden_one = jax.nn.silu(first_pre).astype(jnp.bfloat16)
    second_pre = jnp.dot(hidden_one, layer_two, preferred_element_type=jnp.float32)
    hidden_two = jax.nn.silu(second_pre).astype(jnp.bfloat16)
    return jnp.dot(hidden_two, layer_three, preferred_element_type=jnp.float32)


def surrogate(inputs, layer_one, layer_two, layer_three):
    first_pre = jnp.dot(inputs, layer_one, preferred_element_type=jnp.float32)
    return network_tail(first_pre, layer_two, layer_three)


def merge_total(former, latter):
    counts = former[0] + latter[0]
    change = latter[1] - former[1]
    return (counts, former[1] + change * latter[0] / counts,
            former[2] + latter[2] + change * change * former[0] * latter[0] / counts)


def merge_groups(former, latter):
    counts = former[0] + latter[0]
    change_b = latter[1] - former[1]
    change_d = latter[2] - former[2]
    pair_weight = former[0] * latter[0] / counts
    return (counts, former[1] + change_b * latter[0] / counts, former[2] + change_d * latter[0] / counts,
            former[3] + latter[3] + change_d * change_d * pair_weight,
            former[4] + latter[4] + change_b * change_d * pair_weight)


def reference(base_a, base_b, input_scale, layer_one, layer_two, layer_three, swap_cols, window_ends):
    positions = jnp.arange(D, dtype=jnp.int32)
    row_ids = jnp.arange(WINDOW_ROWS, dtype=jnp.int32)
    firsts = []
    totals = []
    variances = []
    running_total = None
    running_groups = None
    for window in range(WINDOWS):
        inputs_a = (base_a[window].astype(jnp.float32) * input_scale).astype(jnp.bfloat16)
        inputs_b = (base_b[window].astype(jnp.float32) * input_scale).astype(jnp.bfloat16)
        usable = (row_ids < window_ends[window]).astype(jnp.float32)[:, None]
        counts = jnp.sum(usable)
        out_a = surrogate(inputs_a, layer_one, layer_two, layer_three)
        out_b = surrogate(inputs_b, layer_one, layer_two, layer_three)
        pooled_count = 2.0 * counts
        pooled_mean = jnp.sum(usable * (out_a + out_b), axis=0) / pooled_count
        dev_a = out_a - pooled_mean
        dev_b = out_b - pooled_mean
        pooled_spread = jnp.sum(usable * (dev_a * dev_a + dev_b * dev_b), axis=0)
        mean_b = jnp.sum(usable * out_b, axis=0) / counts
        centered_b = usable * (out_b - mean_b)

        def one_group(column):
            chosen = (positions == column)[None, :]
            inputs_c = jnp.where(chosen, inputs_b, inputs_a)
            differ = surrogate(inputs_c, layer_one, layer_two, layer_three) - out_a
            mean_d = jnp.sum(usable * differ, axis=0) / counts
            centered_d = usable * (differ - mean_d)
            return mean_d, jnp.sum(centered_d * centered_d, axis=0), jnp.sum(centered_b * centered_d, axis=0)

        mean_d, spread_d, cross = lax.map(one_group, swap_cols)
        total_state = (pooled_count, pooled_mean, pooled_spread)
        group_state = (counts, mean_b, mean_d, spread_d, cross)
        if window == 0:
            running_total = total_state
            running_groups = group_state
        else:
            running_total = merge_total(running_total, total_state)
            running_groups = merge_groups(running_groups, group_state)
        variance = running_total[2] / running_total[0]
        firsts.append(running_groups[4] / running_groups[0] / variance)
        totals.append(0.5 * (running_groups[3] / running_groups[0] + running_groups[2] * running_groups[2]) / variance)
        variances.append(variance)
    return jnp.stack(firsts), jnp.stack(totals), jnp.stack(variances)
```

```python
import math

import jax
import jax.numpy as jnp
from jax import lax
from jax.experimental import pallas as pl
from jax.experimental.pallas import tpu as pltpu
from jax.sharding import PartitionSpec as P

CHUNK_ROWS = 512
COLUMN_TILE = 256


def dot(left, right):
    return jnp.dot(left, right, preferred_element_type=jnp.float32)


def silu_half(half):
    return half + half * jnp.tanh(half)


def evaluate_kernel(
    front,
    back,
    own_ref,
    *refs,
):
    peers = refs[: front - 1]
    (scale_ref, one_hbm, two_hbm, three_hbm, cols_ref, ends_ref, out_ref) = refs[front - 1 : front + 6]
    (one_ref, two_ref, three_ref, pre_ref, first_ref, second_ref, result_ref, base_ref, sems) = refs[front + 6 :]
    windows, block_rows, width = own_ref.shape[1:]
    hidden = one_ref.shape[1]
    outputs = three_ref.shape[1]
    total_groups = cols_ref.shape[0]
    groups = total_groups // front
    rows = front * windows * block_rows
    copies = [
        pltpu.make_async_copy(source, target, sems.at[index])
        for index, (source, target) in enumerate(
            ((one_hbm, one_ref), (two_hbm, two_ref), (three_hbm, three_ref))
        )
    ]
    for copy in copies:
        copy.start()
    device = lax.axis_index("rows")
    place = device // back
    corner = device % back
    scale = scale_ref[...]
    pieces = [own_ref] + list(peers)

    def scaled(which):
        return jnp.concatenate(
            [(piece[which].reshape(windows * block_rows, width) * scale).astype(jnp.bfloat16) for piece in pieces], 0
        )

    inputs_a = scaled(0)
    inputs_b = scaled(1)
    row_ids = lax.broadcasted_iota(jnp.int32, (groups, width), 0)
    lane_ids = lax.broadcasted_iota(jnp.int32, (groups, width), 1)
    wanted = jnp.zeros((groups, width), jnp.int32)
    for group in range(groups):
        wanted = jnp.where(row_ids == group, cols_ref[place * groups + group], wanted)
    picks = jnp.where(lane_ids == wanted, 1.0, 0.0).astype(jnp.bfloat16)
    contract = (((1,), (1,)), ((), ()))
    delta = 0.5 * (
        lax.dot_general(inputs_b, picks, contract, preferred_element_type=jnp.float32)
        - lax.dot_general(inputs_a, picks, contract, preferred_element_type=jnp.float32)
    )
    copies[0].wait()
    picked = dot(picks, one_ref[...])
    inputs_ab = jnp.concatenate([inputs_a, inputs_b], 0)
    for start in range(0, hidden, COLUMN_TILE):
        tile = slice(start, start + COLUMN_TILE)
        half = 0.5 * dot(inputs_ab, one_ref[:, tile])
        pre_ref[:, tile] = half[:rows]
        first_ref[0, : 2 * rows, tile] = silu_half(half).astype(jnp.bfloat16)
    copies[1].wait()
    copies[2].wait()

    def tail(slot, size):
        for start in range(0, hidden, COLUMN_TILE):
            tile = slice(start, start + COLUMN_TILE)
            half = 0.5 * dot(first_ref[slot, :size], two_ref[:, tile])
            second_ref[slot, :size, tile] = silu_half(half).astype(jnp.bfloat16)
        return dot(second_ref[slot, :size], three_ref[...])

    base_ref[...] = tail(0, 2 * rows)
    out_a = base_ref[:rows]
    out_b = base_ref[rows:]
    sublane = lax.broadcasted_iota(jnp.int32, (block_rows, outputs), 0)
    masks = []
    for peer in range(front):
        member = jnp.bitwise_xor(place, peer) if front & (front - 1) == 0 else lax.rem(place + peer, front)
        first_row = (member * back + corner) * block_rows
        masks.append([jnp.where(sublane + first_row < ends_ref[w], 1.0, 0.0) for w in range(windows)])

    def block(values, peer, window):
        at = (peer * windows + window) * block_rows
        return values[at : at + block_rows]

    for window in range(windows):
        sums = [jnp.zeros((block_rows, outputs), jnp.float32) for _ in range(3)]
        for peer in range(front):
            mask = masks[peer][window]
            va = block(out_a, peer, window)
            vb = block(out_b, peer, window)
            sums[0] += mask * vb
            sums[1] += mask * (va + vb)
            sums[2] += mask * (va * va + vb * vb)
        lines = [jnp.sum(value, axis=0, keepdims=True) for value in sums]
        lines.append(jnp.zeros((8 - len(lines), outputs), jnp.float32))
        out_ref[window, 3 * groups :, :] = jnp.concatenate(lines, 0)

    per_chunk = max(1, min(groups, CHUNK_ROWS // rows))

    def fill(chunk, slot):
        for index in range(per_chunk):
            group = chunk * per_chunk + index
            change = delta[:, group : group + 1]
            for start in range(0, hidden, COLUMN_TILE):
                tile = slice(start, start + COLUMN_TILE)
                half = pre_ref[:, tile] + change * picked[group : group + 1, tile]
                first_ref[slot, index * rows : (index + 1) * rows, tile] = silu_half(half).astype(jnp.bfloat16)

    chunks = groups // per_chunk
    fill(0, 1)
    for chunk in range(chunks):
        slot = (chunk + 1) % 2
        if chunk + 1 < chunks:
            fill(chunk + 1, 1 - slot)
        values = tail(slot, per_chunk * rows)
        for index in range(per_chunk):
            group = chunk * per_chunk + index
            for window in range(windows):
                sums = [jnp.zeros((block_rows, outputs), jnp.float32) for _ in range(3)]
                for peer in range(front):
                    at = index * rows + (peer * windows + window) * block_rows
                    differ = values[at : at + block_rows] - block(base_ref, peer, window)
                    masked = masks[peer][window] * differ
                    sums[0] += masked
                    sums[1] += masked * differ
                    sums[2] += masked * base_ref[pl.ds(rows + (peer * windows + window) * block_rows, block_rows)]
                for kind in range(3):
                    out_ref[window, kind * groups + group : kind * groups + group + 1, :] = jnp.sum(
                        sums[kind], axis=0, keepdims=True
                    )


def conclude_kernel(groups, own_ref, other_ref, ends_ref, out_ref, variance_ref):
    windows = own_ref.shape[0]
    running = jnp.zeros(own_ref.shape[1:], jnp.float32)
    count = jnp.int32(0)
    for window in range(windows):
        running = running + (own_ref[window] + other_ref[window])
        count = count + ends_ref[window]
        share = 1.0 / (jnp.zeros((1, own_ref.shape[2]), jnp.float32) + count.astype(jnp.float32))
        sum_b = running[3 * groups : 3 * groups + 1]
        sum_all = running[3 * groups + 1 : 3 * groups + 2]
        squares = running[3 * groups + 2 : 3 * groups + 3]
        mean = sum_all * (0.5 * share)
        variance = (squares - sum_all * mean) * (0.5 * share)
        mean_d = running[:groups] * share
        weight = share / variance
        out_ref[0, window] = (running[2 * groups : 3 * groups] - sum_b * mean_d) * weight
        out_ref[1, window] = running[groups : 2 * groups] * (0.5 * weight)
        variance_ref[window : window + 1, :] = variance


def assemble_kernel(front, back, own_ref, *refs):
    peers = refs[: front - 1]
    first_ref, total_ref = refs[front - 1 :]
    place = lax.axis_index("rows") // back
    groups = own_ref.shape[2]
    for peer, ref in enumerate([own_ref] + list(peers)):
        member = jnp.bitwise_xor(place, peer) if front & (front - 1) == 0 else lax.rem(place + peer, front)
        start = pl.multiple_of(member * groups, groups)
        first_ref[:, pl.ds(start, groups), :] = ref[0]
        total_ref[:, pl.ds(start, groups), :] = ref[1]


def swap_with(values, pairs):
    return lax.ppermute(values, "rows", pairs)


def local(base_a, base_b, input_scale, layer_one, layer_two, layer_three, swap_cols, window_ends):
    windows, block_rows, width = base_a.shape
    size = lax.axis_size("rows")
    total_groups = swap_cols.shape[0]
    hidden = layer_one.shape[1]
    outputs = layer_three.shape[1]
    back = 2 if size % 2 == 0 else 1
    front = size // back
    groups = total_groups // front
    rows = front * windows * block_rows

    def pairs_of(peer):
        pairs = []
        for device in range(size):
            place, corner = divmod(device, back)
            source = (place ^ peer) if front & (front - 1) == 0 else (place + peer) % front
            pairs.append((source * back + corner, device))
        return pairs

    own = jnp.stack([base_a, base_b]).astype(jnp.float32)
    received = [swap_with(own, pairs_of(peer)) for peer in range(1, front)]
    vmem = pl.BlockSpec(memory_space=pltpu.VMEM)
    smem = pl.BlockSpec(memory_space=pltpu.SMEM)
    anywhere = pl.BlockSpec(memory_space=pl.ANY)
    per_chunk = max(1, min(groups, CHUNK_ROWS // rows))
    room = max(2, per_chunk) * rows
    height = 3 * groups + 8

    def evaluate(*args):
        return evaluate_kernel(front, back, *args)

    partial = pl.pallas_call(
        evaluate,
        out_shape=jax.ShapeDtypeStruct((windows, height, outputs), jnp.float32),
        in_specs=[vmem] * (front + 1) + [anywhere] * 3 + [smem] * 2,
        out_specs=vmem,
        scratch_shapes=[
            pltpu.VMEM(layer_one.shape, jnp.bfloat16),
            pltpu.VMEM(layer_two.shape, jnp.bfloat16),
            pltpu.VMEM(layer_three.shape, jnp.bfloat16),
            pltpu.VMEM((rows, hidden), jnp.float32),
            pltpu.VMEM((2, room, hidden), jnp.bfloat16),
            pltpu.VMEM((2, room, hidden), jnp.bfloat16),
            pltpu.VMEM((room, outputs), jnp.float32),
            pltpu.VMEM((2 * rows, outputs), jnp.float32),
            pltpu.SemaphoreType.DMA((3,)),
        ],
        name="evaluate",
    )(own, *received, input_scale.reshape(1, width), layer_one, layer_two, layer_three, swap_cols, window_ends)

    if back == 2:
        other = swap_with(partial, [(device, device ^ 1) for device in range(size)])
    else:
        other = jnp.zeros_like(partial)

    def conclude(*args):
        return conclude_kernel(groups, *args)

    settled, variance = pl.pallas_call(
        conclude,
        out_shape=(
            jax.ShapeDtypeStruct((2, windows, groups, outputs), jnp.float32),
            jax.ShapeDtypeStruct((windows, outputs), jnp.float32),
        ),
        in_specs=[vmem, vmem, smem],
        out_specs=(vmem, vmem),
        name="conclude",
    )(partial, other, window_ends)

    gathered = [swap_with(settled, pairs_of(peer)) for peer in range(1, front)]

    def assemble(*args):
        return assemble_kernel(front, back, *args)

    whole = jax.ShapeDtypeStruct((windows, total_groups, outputs), jnp.float32)
    first, total = pl.pallas_call(
        assemble,
        out_shape=(whole, whole),
        in_specs=[vmem] * front,
        out_specs=(vmem, vmem),
        name="assemble",
    )(settled, *gathered)
    return first, total, variance


def solution(mesh):
    in_specs = (P(None, "rows", None), P(None, "rows", None), P(), P(), P(), P(), P("par"), P())
    out_specs = (P(None, "par", None), P(None, "par", None), P())
    return jax.shard_map(local, mesh=mesh, in_specs=in_specs, out_specs=out_specs, check_vma=False)
```

```python
import math

import jax
import jax.numpy as jnp
from jax import lax
from jax.experimental import pallas as pl
from jax.experimental.pallas import tpu as pltpu
from jax.sharding import PartitionSpec as P

CHUNK_ROWS = 576
COLUMN_TILE = 256
SPARE_BYTES = 10 * 1024 * 1024


def dot(left, right):
    return jnp.dot(left, right, preferred_element_type=jnp.float32)


def silu_half(half):
    return half + half * jnp.tanh(half)


def units_per_chunk(units, rows):
    return max(count for count in range(1, units + 1) if units % count == 0 and (count == 1 or count * rows <= CHUNK_ROWS))


def member_of(place, peer, front):
    return jnp.bitwise_xor(place, peer) if front & (front - 1) == 0 else lax.rem(place + peer, front)


def networks(pieces, mask_of, scale, picks, one_ref, wait_one, two_ref, three_ref, wait_rest, base_sums, out_ref, scratch):
    pre_ref, first_ref, second_ref, result_ref, base_ref = scratch
    windows, block_rows, width = pieces[0].shape[1:]
    groups = picks.shape[0]
    hidden = one_ref.shape[1]
    outputs = three_ref.shape[1]
    rows = len(pieces) * windows * block_rows

    def scaled(which):
        return jnp.concatenate(
            [(piece[which].reshape(windows * block_rows, width) * scale).astype(jnp.bfloat16) for piece in pieces], 0
        )

    inputs_a = scaled(0)
    inputs_b = scaled(1)
    contract = (((1,), (1,)), ((), ()))
    delta = 0.5 * (
        lax.dot_general(inputs_b, picks, contract, preferred_element_type=jnp.float32)
        - lax.dot_general(inputs_a, picks, contract, preferred_element_type=jnp.float32)
    )
    wait_one()
    picked = dot(picks, one_ref[...])
    inputs_ab = jnp.concatenate([inputs_a, inputs_b], 0)
    for start in range(0, hidden, COLUMN_TILE):
        tile = slice(start, start + COLUMN_TILE)
        pre_ref[:, tile] = 0.5 * dot(inputs_ab, one_ref[:, tile])

    units = groups + 2
    per_chunk = units_per_chunk(units, rows)

    def fill(chunk):
        for index in range(per_chunk):
            unit = chunk * per_chunk + index
            for start in range(0, hidden, COLUMN_TILE):
                tile = slice(start, start + COLUMN_TILE)
                half = pre_ref[rows : 2 * rows, tile] if unit == 1 else pre_ref[:rows, tile]
                if unit >= 2:
                    group = unit - 2
                    half = half + delta[:, group : group + 1] * picked[group : group + 1, tile]
                first_ref[chunk % 2, index * rows : (index + 1) * rows, tile] = silu_half(half).astype(jnp.bfloat16)

    def tail(chunk):
        for start in range(0, hidden, COLUMN_TILE):
            tile = slice(start, start + COLUMN_TILE)
            half = 0.5 * dot(first_ref[chunk % 2], two_ref[:, tile])
            second_ref[chunk % 2, :, tile] = silu_half(half).astype(jnp.bfloat16)
        return dot(second_ref[chunk % 2], three_ref[...])

    def block_at(peer, window):
        return (peer * windows + window) * block_rows

    def total(value):
        return jnp.sum(value, axis=0, keepdims=True)

    chunks = units // per_chunk
    fill(0)
    wait_rest()
    for chunk in range(chunks):
        if chunk + 1 < chunks:
            fill(chunk + 1)
        result_ref[chunk % 2] = tail(chunk)
        for index in range(per_chunk):
            unit = chunk * per_chunk + index
            if unit < 2:
                base_ref[unit] = result_ref[chunk % 2, index * rows : (index + 1) * rows]
                if unit == 1:
                    for window in range(windows):
                        sums = [jnp.zeros((block_rows, outputs), jnp.float32) for _ in range(3)]
                        for peer in range(len(pieces)):
                            mask = mask_of(peer, window)
                            at = block_at(peer, window)
                            va = base_ref[0, at : at + block_rows]
                            vb = base_ref[1, at : at + block_rows]
                            sums[0] += mask * vb
                            sums[1] += mask * (va + vb)
                            sums[2] += mask * (va * va + vb * vb)
                        base_sums(window, [total(value) for value in sums])
                continue
            group = unit - 2
            for window in range(windows):
                sums = [jnp.zeros((block_rows, outputs), jnp.float32) for _ in range(3)]
                for peer in range(len(pieces)):
                    at = block_at(peer, window)
                    here = index * rows + at
                    differ = result_ref[chunk % 2, here : here + block_rows] - base_ref[0, at : at + block_rows]
                    masked = mask_of(peer, window) * differ
                    sums[0] += masked
                    sums[1] += masked * differ
                    sums[2] += masked * base_ref[1, at : at + block_rows]
                for kind in range(3):
                    out_ref(window, kind * groups + group, total(sums[kind]))


def early_kernel(
    front, back, own_ref, scale_hbm, one_hbm, two_hbm, three_hbm, cols_hbm, ends_hbm,
    out_ref, scale_ref, one_ref, two_ref, three_ref, picks_ref, masks_ref, cols_ref, ends_ref, sems, *scratch,
):
    moves = (
        (cols_hbm, cols_ref),
        (ends_hbm, ends_ref),
        (scale_hbm, scale_ref),
        (one_hbm, one_ref),
        (two_hbm, two_ref),
        (three_hbm, three_ref),
    )
    copies = [pltpu.make_async_copy(source, target, sems.at[index]) for index, (source, target) in enumerate(moves)]
    for copy in copies:
        copy.start()
    for copy in copies[:3]:
        copy.wait()
    windows, block_rows, width = own_ref.shape[1:]
    groups = picks_ref.shape[0]
    outputs = three_ref.shape[1]
    device = lax.axis_index("rows")
    place = device // back
    corner = device % back
    row_ids = lax.broadcasted_iota(jnp.int32, (groups, width), 0)
    lane_ids = lax.broadcasted_iota(jnp.int32, (groups, width), 1)
    wanted = jnp.zeros((groups, width), jnp.int32)
    for group in range(groups):
        wanted = jnp.where(row_ids == group, cols_ref[place * groups + group], wanted)
    picks = jnp.where(lane_ids == wanted, 1.0, 0.0).astype(jnp.bfloat16)
    picks_ref[...] = picks
    sublane = lax.broadcasted_iota(jnp.int32, (block_rows, outputs), 0)
    own_masks = []
    for peer in range(front):
        first_row = (member_of(place, peer, front) * back + corner) * block_rows
        for window in range(windows):
            mask = jnp.where(sublane + first_row < ends_ref[window], 1.0, 0.0)
            if peer == 0:
                own_masks.append(mask)
            else:
                masks_ref[peer - 1, window] = mask
    counts = []
    count = jnp.int32(0)
    for window in range(windows):
        count = count + ends_ref[window]
        counts.append(count)

    def base_sums(window, lines):
        lines = lines + [jnp.zeros((1, outputs), jnp.float32) + counts[window].astype(jnp.float32)]
        lines.append(jnp.zeros((8 - len(lines), outputs), jnp.float32))
        out_ref[window, 3 * groups :, :] = jnp.concatenate(lines, 0)

    def store(window, line, value):
        out_ref[window, line : line + 1, :] = value

    def wait_rest():
        copies[4].wait()
        copies[5].wait()

    networks(
        [own_ref], lambda peer, window: own_masks[window], scale_ref[...], picks, one_ref, copies[3].wait,
        two_ref, three_ref, wait_rest, base_sums, store, scratch,
    )


def late_kernel(front, *refs):
    pieces = refs[: front - 1]
    scale_ref, one_ref, two_ref, three_ref, picks_ref, masks_ref, early_ref, out_ref = refs[front - 1 : front + 7]
    scratch = refs[front + 7 :]
    groups = picks_ref.shape[0]

    def base_sums(window, lines):
        for index, line in enumerate(lines):
            store(window, 3 * groups + index, line)
        rest = slice(3 * groups + len(lines), None)
        out_ref[window, rest, :] = early_ref[window, rest, :]

    def store(window, line, value):
        out_ref[window, line : line + 1, :] = early_ref[window, line : line + 1, :] + value

    def nothing():
        return None

    networks(
        list(pieces), lambda peer, window: masks_ref[peer, window], scale_ref[...], picks_ref[...], one_ref, nothing,
        two_ref, three_ref, nothing, base_sums, store, scratch,
    )


def conclude_kernel(groups, own_ref, other_ref, out_ref, variance_ref):
    windows = own_ref.shape[0]
    running = jnp.zeros(own_ref.shape[1:], jnp.float32)
    for window in range(windows):
        running = running + (own_ref[window] + other_ref[window])
        share = 1.0 / own_ref[window, 3 * groups + 3 : 3 * groups + 4]
        sum_b = running[3 * groups : 3 * groups + 1]
        sum_all = running[3 * groups + 1 : 3 * groups + 2]
        squares = running[3 * groups + 2 : 3 * groups + 3]
        mean = sum_all * (0.5 * share)
        variance = (squares - sum_all * mean) * (0.5 * share)
        mean_d = running[:groups] * share
        weight = share / variance
        out_ref[0, window] = (running[2 * groups : 3 * groups] - sum_b * mean_d) * weight
        out_ref[1, window] = running[groups : 2 * groups] * (0.5 * weight)
        variance_ref[window : window + 1, :] = variance


def assemble_kernel(front, back, own_ref, *refs):
    peers = refs[: front - 1]
    settled_ref, first_ref, total_ref, variance_ref = refs[front - 1 :]
    place = lax.axis_index("rows") // back
    groups = own_ref.shape[2]
    for peer, ref in enumerate([own_ref] + list(peers)):
        start = pl.multiple_of(member_of(place, peer, front) * groups, groups)
        first_ref[:, pl.ds(start, groups), :] = ref[0]
        total_ref[:, pl.ds(start, groups), :] = ref[1]
    variance_ref[...] = settled_ref[...]


def near(values):
    return pltpu.with_memory_space_constraint(values, pltpu.VMEM)


def far(values):
    return pltpu.with_memory_space_constraint(values, pltpu.HBM)


def exchange(values, pairs):
    return lax.ppermute(values, "rows", pairs)


def local(base_a, base_b, input_scale, layer_one, layer_two, layer_three, swap_cols, window_ends):
    windows, block_rows, width = base_a.shape
    size = lax.axis_size("rows")
    total_groups = swap_cols.shape[0]
    hidden = layer_one.shape[1]
    outputs = layer_three.shape[1]
    back = 2 if size % 2 == 0 else 1
    front = size // back
    groups = total_groups // front
    height = 3 * groups + 8

    def pairs_of(peer):
        pairs = []
        for device in range(size):
            place, corner = divmod(device, back)
            source = (place ^ peer) if front & (front - 1) == 0 else (place + peer) % front
            pairs.append((source * back + corner, device))
        return pairs

    vmem = pl.BlockSpec(memory_space=pltpu.VMEM)
    anywhere = pl.BlockSpec(memory_space=pl.ANY)

    def scratch_of(count):
        rows = count * windows * block_rows
        chunk = units_per_chunk(groups + 2, rows) * rows
        return [
            pltpu.VMEM((2 * rows, hidden), jnp.float32),
            pltpu.VMEM((2, chunk, hidden), jnp.bfloat16),
            pltpu.VMEM((2, chunk, hidden), jnp.bfloat16),
            pltpu.VMEM((2, chunk, outputs), jnp.float32),
            pltpu.VMEM((2, rows, outputs), jnp.float32),
        ]

    def room_of(count):
        held = sum(math.prod(space.shape) * jnp.dtype(space.dtype).itemsize for space in scratch_of(count))
        return pltpu.CompilerParams(vmem_limit_bytes=held + SPARE_BYTES)

    def work_of(count):
        rows = count * windows * block_rows * (groups + 2)
        return pl.CostEstimate(
            flops=2 * rows * hidden * (hidden + outputs),
            transcendentals=2 * rows * hidden,
            bytes_accessed=2 * (layer_one.size + layer_two.size + layer_three.size),
        )

    own = jnp.stack([base_a, base_b]).astype(jnp.float32)
    received = [exchange(own, pairs_of(peer)) for peer in range(1, front)]
    scale = input_scale.reshape(1, width)

    def early(*args):
        return early_kernel(front, back, *args)

    sums, scales, one, two, three, picks, masks = pl.pallas_call(
        early,
        out_shape=(
            pltpu.VMEM((windows, height, outputs), jnp.float32),
            pltpu.VMEM(scale.shape, scale.dtype),
            pltpu.VMEM(layer_one.shape, layer_one.dtype),
            pltpu.VMEM(layer_two.shape, layer_two.dtype),
            pltpu.VMEM(layer_three.shape, layer_three.dtype),
            pltpu.VMEM((groups, width), jnp.bfloat16),
            pltpu.VMEM((front - 1, windows, block_rows, outputs), jnp.float32),
        ),
        in_specs=[vmem] + [anywhere] * 6,
        out_specs=(vmem,) * 7,
        scratch_shapes=[
            pltpu.SMEM(swap_cols.shape, swap_cols.dtype),
            pltpu.SMEM(window_ends.shape, window_ends.dtype),
            pltpu.SemaphoreType.DMA((6,)),
            *scratch_of(1),
        ],
        cost_estimate=work_of(1),
        compiler_params=room_of(1),
        name="early",
    )(near(own), *(far(value) for value in (scale, layer_one, layer_two, layer_three, swap_cols, window_ends)))

    def late(*args):
        return late_kernel(front, *args)

    partial = pl.pallas_call(
        late,
        out_shape=pltpu.VMEM((windows, height, outputs), jnp.float32),
        in_specs=[vmem] * (front + 6),
        out_specs=vmem,
        scratch_shapes=scratch_of(front - 1),
        cost_estimate=work_of(front - 1),
        compiler_params=room_of(front - 1),
        name="late",
    )(*(near(value) for value in (*received, scales, one, two, three, picks, masks, sums)))

    if back == 2:
        other = exchange(partial, [(device, device ^ 1) for device in range(size)])
    else:
        other = jnp.zeros_like(partial)

    def conclude(*args):
        return conclude_kernel(groups, *args)

    settled, variance = pl.pallas_call(
        conclude,
        out_shape=(
            pltpu.VMEM((2, windows, groups, outputs), jnp.float32),
            pltpu.VMEM((windows, outputs), jnp.float32),
        ),
        in_specs=[vmem, vmem],
        out_specs=(vmem, vmem),
        compiler_params=pltpu.CompilerParams(vmem_limit_bytes=SPARE_BYTES),
        name="conclude",
    )(near(partial), near(other))

    gathered = [exchange(settled, pairs_of(peer)) for peer in range(1, front)]

    def assemble(*args):
        return assemble_kernel(front, back, *args)

    whole = jax.ShapeDtypeStruct((windows, total_groups, outputs), jnp.float32)
    return pl.pallas_call(
        assemble,
        out_shape=(whole, whole, jax.ShapeDtypeStruct((windows, outputs), jnp.float32)),
        in_specs=[vmem] * (front + 1),
        out_specs=(vmem, vmem, vmem),
        compiler_params=pltpu.CompilerParams(vmem_limit_bytes=SPARE_BYTES),
        name="assemble",
    )(*(near(value) for value in (settled, *gathered, variance)))


def solution(mesh):
    in_specs = (P(None, "rows", None), P(None, "rows", None), P(), P(), P(), P(), P("par"), P())
    out_specs = (P(None, "par", None), P(None, "par", None), P())
    return jax.shard_map(local, mesh=mesh, in_specs=in_specs, out_specs=out_specs, check_vma=False)
```

```python
import math

import jax
import jax.numpy as jnp
from jax import lax
from jax.experimental import pallas as pl
from jax.experimental.pallas import tpu as pltpu
from jax.sharding import PartitionSpec as P

CHUNK_ROWS = 576
COLUMN_TILE = 256
PASS_FLOPS = 4_000_000_000
SPARE_BYTES = 10 * 1024 * 1024


def dot(left, right):
    return jnp.dot(left, right, preferred_element_type=jnp.float32)


def silu_half(half):
    return half + half * jnp.tanh(half)


def units_per_chunk(units, rows):
    return max(count for count in range(1, units + 1) if units % count == 0 and (count == 1 or count * rows <= CHUNK_ROWS))


def member_of(place, peer, front):
    return jnp.bitwise_xor(place, peer) if front & (front - 1) == 0 else lax.rem(place + peer, front)


def total(value):
    return jnp.sum(value, axis=0, keepdims=True)


def prepare(pieces, scale, picks, one_ref, pre_ref):
    windows, block_rows, width = pieces[0].shape[1:]
    hidden = one_ref.shape[1]

    def scaled(which):
        return jnp.concatenate(
            [(piece[which].reshape(windows * block_rows, width) * scale).astype(jnp.bfloat16) for piece in pieces], 0
        )

    inputs_a = scaled(0)
    inputs_b = scaled(1)
    contract = (((1,), (1,)), ((), ()))
    delta = 0.5 * (
        lax.dot_general(inputs_b, picks, contract, preferred_element_type=jnp.float32)
        - lax.dot_general(inputs_a, picks, contract, preferred_element_type=jnp.float32)
    )
    picked = dot(picks, one_ref[...])
    inputs_ab = jnp.concatenate([inputs_a, inputs_b], 0)
    for start in range(0, hidden, COLUMN_TILE):
        tile = slice(start, start + COLUMN_TILE)
        pre_ref[:, tile] = 0.5 * dot(inputs_ab, one_ref[:, tile])
    return delta, picked


def fill(units, rows, pre_ref, delta, picked, filled_ref):
    hidden = pre_ref.shape[1]
    for index, unit in enumerate(units):
        for start in range(0, hidden, COLUMN_TILE):
            tile = slice(start, start + COLUMN_TILE)
            half = pre_ref[rows : 2 * rows, tile] if unit == 1 else pre_ref[:rows, tile]
            if unit >= 2:
                group = unit - 2
                half = half + delta[:, group : group + 1] * picked[group : group + 1, tile]
            filled_ref[index * rows : (index + 1) * rows, tile] = silu_half(half).astype(jnp.bfloat16)


def tail(filled_ref, second_ref, two_ref, three_ref):
    hidden = two_ref.shape[1]
    for start in range(0, hidden, COLUMN_TILE):
        tile = slice(start, start + COLUMN_TILE)
        half = 0.5 * dot(filled_ref[...], two_ref[:, tile])
        second_ref[:, tile] = silu_half(half).astype(jnp.bfloat16)
    return dot(second_ref[...], three_ref[...])


def tally(units, count, windows, block_rows, mask_of, result_ref, base_ref, base_sums, store):
    outputs = result_ref.shape[1]
    rows = count * windows * block_rows
    zero = jnp.zeros((block_rows, outputs), jnp.float32)
    for index, unit in enumerate(units):
        if unit < 2:
            base_ref[unit] = result_ref[index * rows : (index + 1) * rows]
            if unit == 0:
                continue
        for window in range(windows):
            sums = [zero, zero, zero]
            for peer in range(count):
                at = (peer * windows + window) * block_rows
                mask = mask_of(peer, window)
                va = base_ref[0, at : at + block_rows]
                vb = base_ref[1, at : at + block_rows]
                if unit == 1:
                    sums[0] += mask * vb
                    sums[1] += mask * (va + vb)
                    sums[2] += mask * (va * va + vb * vb)
                else:
                    differ = result_ref[index * rows + at : index * rows + at + block_rows] - va
                    masked = mask * differ
                    sums[0] += masked
                    sums[1] += masked * differ
                    sums[2] += masked * vb
            lines = [total(value) for value in sums]
            if unit == 1:
                base_sums(window, lines)
            else:
                store(unit - 2, window, lines)


def line_at(groups, group, window, kind):
    return (window * 3 + kind) * groups + group


def pass_kernel(given_ref, out_ref):
    pass


def early_kernel(
    front, own_ref, scale_ref, one_ref, two_ref, three_ref, cols_ref, ends_ref, out_ref, picks_ref, masks_ref,
    pre_ref, first_ref, second_ref, result_ref, base_ref,
):
    windows, block_rows, width = own_ref.shape[1:]
    groups = picks_ref.shape[0]
    outputs = three_ref.shape[1]
    device = lax.axis_index("rows")
    place = lax.rem(device, front)
    corner = device // front
    total_groups = cols_ref.shape[1]
    line_ids = lax.broadcasted_iota(jnp.int32, (groups, total_groups), 0)
    spot_ids = lax.broadcasted_iota(jnp.int32, (groups, total_groups), 1)
    mine = jnp.where(spot_ids == line_ids + place * groups, cols_ref[...].astype(jnp.float32), 0.0)
    wanted = jnp.sum(mine, axis=1, keepdims=True).astype(jnp.int32)
    lane_ids = lax.broadcasted_iota(jnp.int32, (groups, width), 1)
    picks_ref[...] = jnp.where(lane_ids == wanted, 1.0, 0.0).astype(jnp.bfloat16)
    sublane = lax.broadcasted_iota(jnp.int32, (block_rows, outputs), 0)
    ends = [jnp.broadcast_to(ends_ref[0:1, window : window + 1], (block_rows, outputs)) for window in range(windows)]
    for peer in range(front):
        first_row = (corner * front + member_of(place, peer, front)) * block_rows
        for window in range(windows):
            masks_ref[peer, window] = jnp.where(sublane + first_row < ends[window], 1.0, 0.0)
    counts = []
    for window in range(windows):
        counts.append(ends[window][0:1].astype(jnp.float32) + (counts[-1] if counts else 0.0))

    def base_sums(window, lines):
        lines = lines + [counts[window]]
        start = 3 * windows * groups + 4 * window
        out_ref[start : start + 4, :] = jnp.concatenate(lines, 0)

    def store(group, window, lines):
        for kind in range(3):
            at = line_at(groups, group, window, kind)
            out_ref[at : at + 1, :] = lines[kind]

    rows = windows * block_rows
    units = range(groups + 2)
    delta, picked = prepare([own_ref], scale_ref[...], picks_ref[...], one_ref, pre_ref)
    fill(units, rows, pre_ref, delta, picked, first_ref)
    result_ref[...] = tail(first_ref, second_ref, two_ref, three_ref)
    tally(
        units, 1, windows, block_rows, lambda peer, window: masks_ref[0, window], result_ref, base_ref, base_sums, store
    )


def late_kernel(front, chunks, *refs):
    pieces = refs[: front - 1]
    (scale_ref, one_ref, two_ref, three_ref, picks_ref, masks_ref, early_ref, out_ref) = refs[front - 1 : front + 7]
    (pre_ref, first_ref, second_ref, result_ref, base_ref) = refs[front + 7 :]
    windows, block_rows = pieces[0].shape[1:3]
    groups = picks_ref.shape[0]
    rows = (front - 1) * windows * block_rows
    stats = 3 * windows * groups

    def mask_of(peer, window):
        return masks_ref[peer + 1, window]

    def base_sums(window, lines):
        at = stats + 4 * window
        out_ref[at : at + 3, :] = early_ref[at : at + 3, :] + jnp.concatenate(lines, 0)
        out_ref[at + 3 : at + 4, :] = early_ref[at + 3 : at + 4, :]

    def store(group, window, lines):
        for kind in range(3):
            at = line_at(groups, group, window, kind)
            out_ref[at : at + 1, :] = early_ref[at : at + 1, :] + lines[kind]

    delta, picked = prepare(list(pieces), scale_ref[...], picks_ref[...], one_ref, pre_ref)
    fill(chunks[0], rows, pre_ref, delta, picked, first_ref.at[0])
    for index, units in enumerate(chunks):
        slot = index % 2
        if index + 1 < len(chunks):
            fill(chunks[index + 1], rows, pre_ref, delta, picked, first_ref.at[1 - slot])
        result_ref[slot] = tail(first_ref.at[slot], second_ref.at[slot], two_ref, three_ref)
        tally(units, front - 1, windows, block_rows, mask_of, result_ref.at[slot], base_ref, base_sums, store)


def conclude_kernel(own_ref, other_ref, out_ref, variance_ref):
    windows, groups = out_ref.shape[1:3]
    stats = 3 * windows * groups
    running = None
    for window in range(windows):
        at = stats + 4 * window
        pieces = [own_ref[at : at + 3] + other_ref[at : at + 3]]
        for kind in range(3):
            line = line_at(groups, 0, window, kind)
            pieces.append(own_ref[line : line + groups] + other_ref[line : line + groups])
        running = pieces if running is None else [former + latter for former, latter in zip(running, pieces)]
        share = 1.0 / own_ref[at + 3 : at + 4]
        base, sum_d, squares_d, cross = running
        mean = base[1:2] * (0.5 * share)
        variance = (base[2:3] - base[1:2] * mean) * (0.5 * share)
        weight = share / variance
        out_ref[0, window] = (cross - (base[0:1] * share) * sum_d) * weight
        out_ref[1, window] = squares_d * (0.5 * weight)
        variance_ref[window : window + 1, :] = variance


def assemble_kernel(front, own_ref, *refs):
    peers = refs[: front - 1]
    settled_ref, first_ref, total_ref, variance_ref = refs[front - 1 :]
    place = lax.rem(lax.axis_index("rows"), front)
    groups = own_ref.shape[2]
    for peer, ref in enumerate([own_ref] + list(peers)):
        start = pl.multiple_of(member_of(place, peer, front) * groups, groups)
        first_ref[:, pl.ds(start, groups), :] = ref[0]
        total_ref[:, pl.ds(start, groups), :] = ref[1]
    variance_ref[...] = settled_ref[...]


def near(values):
    return pltpu.with_memory_space_constraint(values, pltpu.VMEM)


def exchange(values, pairs):
    return lax.ppermute(values, "rows", pairs)


def local(base_a, base_b, input_scale, layer_one, layer_two, layer_three, swap_cols, window_ends):
    windows, block_rows, width = base_a.shape
    size = lax.axis_size("rows")
    total_groups = swap_cols.shape[0]
    hidden = layer_one.shape[1]
    outputs = layer_three.shape[1]
    back = 2 if size % 2 == 0 else 1
    front = size // back
    groups = total_groups // front
    late_rows = (front - 1) * windows * block_rows
    per_chunk = units_per_chunk(groups + 2, late_rows)
    chunks = [range(at, at + per_chunk) for at in range(0, groups + 2, per_chunk)]
    height = (3 * groups + 4) * windows

    def pairs_of(peer):
        pairs = []
        for device in range(size):
            corner, place = divmod(device, front)
            source = (place ^ peer) if front & (front - 1) == 0 else (place + peer) % front
            pairs.append((corner * front + source, device))
        return pairs

    vmem = pl.BlockSpec(memory_space=pltpu.VMEM)

    def room_of(spaces):
        held = sum(math.prod(space.shape) * jnp.dtype(space.dtype).itemsize for space in spaces)
        return pltpu.CompilerParams(vmem_limit_bytes=held + SPARE_BYTES)

    def work_of(rows):
        return pl.CostEstimate(
            flops=2 * rows * hidden * (hidden + outputs),
            transcendentals=2 * rows * hidden,
            bytes_accessed=2 * (layer_one.size + layer_two.size + layer_three.size),
        )

    own = jnp.stack([base_a, base_b]).astype(jnp.float32)
    own = pl.pallas_call(
        pass_kernel,
        out_shape=pltpu.VMEM(own.shape, own.dtype),
        in_specs=[pl.BlockSpec(memory_space=pltpu.VMEM)],
        out_specs=pl.BlockSpec(memory_space=pltpu.VMEM),
        input_output_aliases={0: 0},
        cost_estimate=pl.CostEstimate(flops=PASS_FLOPS, transcendentals=0, bytes_accessed=0),
        compiler_params=pltpu.CompilerParams(vmem_limit_bytes=1024 * 1024),
        name="pass",
    )(near(own))
    own = near(own)
    received = [exchange(own, pairs_of(peer)) for peer in range(1, front)]
    scale = input_scale.reshape(1, width)
    scales, one, two, three = near(scale), near(layer_one), near(layer_two), near(layer_three)

    def early(*args):
        return early_kernel(front, *args)

    own_rows = windows * block_rows
    early_rows = (groups + 2) * own_rows
    early_scratch = [
        pltpu.VMEM((2 * own_rows, hidden), jnp.float32),
        pltpu.VMEM((early_rows, hidden), jnp.bfloat16),
        pltpu.VMEM((early_rows, hidden), jnp.bfloat16),
        pltpu.VMEM((early_rows, outputs), jnp.float32),
        pltpu.VMEM((2, own_rows, outputs), jnp.float32),
    ]
    sums, picks, masks = pl.pallas_call(
        early,
        out_shape=(
            pltpu.VMEM((height, outputs), jnp.float32),
            pltpu.VMEM((groups, width), jnp.bfloat16),
            pltpu.VMEM((front, windows, block_rows, outputs), jnp.float32),
        ),
        in_specs=[vmem] * 7,
        out_specs=(vmem,) * 3,
        scratch_shapes=early_scratch,
        cost_estimate=work_of(early_rows),
        compiler_params=room_of(early_scratch),
        name="early",
    )(
        own,
        scales,
        one,
        two,
        three,
        near(swap_cols.reshape(1, total_groups)),
        near(window_ends.reshape(1, windows)),
    )

    def late(*args):
        return late_kernel(front, chunks, *args)

    chunk_rows = per_chunk * late_rows
    late_scratch = [
        pltpu.VMEM((2 * late_rows, hidden), jnp.float32),
        pltpu.VMEM((2, chunk_rows, hidden), jnp.bfloat16),
        pltpu.VMEM((2, chunk_rows, hidden), jnp.bfloat16),
        pltpu.VMEM((2, chunk_rows, outputs), jnp.float32),
        pltpu.VMEM((2, late_rows, outputs), jnp.float32),
    ]
    partial = pl.pallas_call(
        late,
        out_shape=pltpu.VMEM((height, outputs), jnp.float32),
        in_specs=[vmem] * (front + 6),
        out_specs=vmem,
        scratch_shapes=late_scratch,
        cost_estimate=work_of(len(chunks) * chunk_rows),
        compiler_params=room_of(late_scratch),
        name="late",
    )(*(near(value) for value in (*received, scales, one, two, three, picks, masks, sums)))
    partial = near(partial)
    if back == 1:
        other = jnp.zeros_like(partial)
    else:
        other = exchange(partial, [(device, (device + front) % size) for device in range(size)])

    settled, variance = pl.pallas_call(
        conclude_kernel,
        out_shape=(
            pltpu.VMEM((2, windows, groups, outputs), jnp.float32),
            pltpu.VMEM((windows, outputs), jnp.float32),
        ),
        in_specs=[vmem, vmem],
        out_specs=(vmem, vmem),
        compiler_params=pltpu.CompilerParams(vmem_limit_bytes=SPARE_BYTES),
        name="conclude",
    )(partial, near(other))

    gathered = [exchange(settled, pairs_of(peer)) for peer in range(1, front)]

    def assemble(*args):
        return assemble_kernel(front, *args)

    whole = jax.ShapeDtypeStruct((windows, total_groups, outputs), jnp.float32)
    return pl.pallas_call(
        assemble,
        out_shape=(whole, whole, jax.ShapeDtypeStruct((windows, outputs), jnp.float32)),
        in_specs=[vmem] * (front + 1),
        out_specs=(vmem, vmem, vmem),
        compiler_params=pltpu.CompilerParams(vmem_limit_bytes=SPARE_BYTES),
        name="assemble",
    )(*(near(value) for value in (settled, *gathered, variance)))


def solution(mesh):
    in_specs = (P(None, "rows", None), P(None, "rows", None), P(), P(), P(), P(), P("par"), P())
    out_specs = (P(None, "par", None), P(None, "par", None), P())
    return jax.shard_map(local, mesh=mesh, in_specs=in_specs, out_specs=out_specs, check_vma=False)
```

```python
import math

import jax
import jax.numpy as jnp
from jax import lax
from jax.experimental import pallas as pl
from jax.experimental.pallas import tpu as pltpu
from jax.sharding import PartitionSpec as P

CHUNK_ROWS = 576
COLUMN_TILE = 256
PASS_FLOPS = 4_000_000_000
SPARE_BYTES = 10 * 1024 * 1024


def dot(left, right):
    return jnp.dot(left, right, preferred_element_type=jnp.float32)


def silu_half(half):
    return half + half * jnp.tanh(half)


def units_per_chunk(units, rows):
    return max(count for count in range(1, units + 1) if units % count == 0 and (count == 1 or count * rows <= CHUNK_ROWS))


def order_of(front):
    peers = list(range(1, front))
    return peers[1:2] + peers[:1] + peers[2:]


def member_of(place, peer, front):
    return jnp.bitwise_xor(place, peer) if front & (front - 1) == 0 else lax.rem(place + peer, front)


def total(value):
    return jnp.sum(value, axis=0, keepdims=True)


def prepare(pieces, scale, picks, one_ref, pre_ref):
    windows, block_rows, width = pieces[0].shape[1:]
    hidden = one_ref.shape[1]

    def scaled(which):
        return jnp.concatenate(
            [(piece[which].reshape(windows * block_rows, width) * scale).astype(jnp.bfloat16) for piece in pieces], 0
        )

    inputs_a = scaled(0)
    inputs_b = scaled(1)
    contract = (((1,), (1,)), ((), ()))
    delta = 0.5 * (
        lax.dot_general(inputs_b, picks, contract, preferred_element_type=jnp.float32)
        - lax.dot_general(inputs_a, picks, contract, preferred_element_type=jnp.float32)
    )
    picked = dot(picks, one_ref[...])
    inputs_ab = jnp.concatenate([inputs_a, inputs_b], 0)
    for start in range(0, hidden, COLUMN_TILE):
        tile = slice(start, start + COLUMN_TILE)
        pre_ref[:, tile] = 0.5 * dot(inputs_ab, one_ref[:, tile])
    return delta, picked


def fill(units, rows, pre_ref, delta, picked, filled_ref):
    hidden = pre_ref.shape[1]
    for index, unit in enumerate(units):
        for start in range(0, hidden, COLUMN_TILE):
            tile = slice(start, start + COLUMN_TILE)
            half = pre_ref[rows : 2 * rows, tile] if unit == 1 else pre_ref[:rows, tile]
            if unit >= 2:
                group = unit - 2
                half = half + delta[:, group : group + 1] * picked[group : group + 1, tile]
            filled_ref[index * rows : (index + 1) * rows, tile] = silu_half(half).astype(jnp.bfloat16)


def tail(filled_ref, second_ref, two_ref, three_ref):
    hidden = two_ref.shape[1]
    for start in range(0, hidden, COLUMN_TILE):
        tile = slice(start, start + COLUMN_TILE)
        half = 0.5 * dot(filled_ref[...], two_ref[:, tile])
        second_ref[:, tile] = silu_half(half).astype(jnp.bfloat16)
    return dot(second_ref[...], three_ref[...])


def tally(units, count, windows, block_rows, mask_of, result_ref, base_ref, base_sums, store):
    outputs = result_ref.shape[1]
    rows = count * windows * block_rows
    zero = jnp.zeros((block_rows, outputs), jnp.float32)
    for index, unit in enumerate(units):
        if unit < 2:
            base_ref[unit] = result_ref[index * rows : (index + 1) * rows]
            if unit == 0:
                continue
        for window in range(windows):
            sums = [zero, zero, zero]
            for peer in range(count):
                at = (peer * windows + window) * block_rows
                mask = mask_of(peer, window)
                va = base_ref[0, at : at + block_rows]
                vb = base_ref[1, at : at + block_rows]
                if unit == 1:
                    sums[0] += mask * vb
                    sums[1] += mask * (va + vb)
                    sums[2] += mask * (va * va + vb * vb)
                else:
                    differ = result_ref[index * rows + at : index * rows + at + block_rows] - va
                    masked = mask * differ
                    sums[0] += masked
                    sums[1] += masked * differ
                    sums[2] += masked * vb
            lines = [total(value) for value in sums]
            if unit == 1:
                base_sums(window, lines)
            else:
                store(unit - 2, window, lines)


def line_at(groups, group, window, kind):
    return (window * 3 + kind) * groups + group


def pass_kernel(given_ref, out_ref):
    pass


def early_kernel(
    front, own_ref, scale_ref, one_ref, two_ref, three_ref, cols_ref, ends_ref, out_ref, picks_ref, masks_ref,
    pre_ref, first_ref, second_ref, result_ref, base_ref,
):
    windows, block_rows, width = own_ref.shape[1:]
    groups = picks_ref.shape[0]
    outputs = three_ref.shape[1]
    device = lax.axis_index("rows")
    place = lax.rem(device, front)
    corner = device // front
    total_groups = cols_ref.shape[1]
    line_ids = lax.broadcasted_iota(jnp.int32, (groups, total_groups), 0)
    spot_ids = lax.broadcasted_iota(jnp.int32, (groups, total_groups), 1)
    mine = jnp.where(spot_ids == line_ids + place * groups, cols_ref[...].astype(jnp.float32), 0.0)
    wanted = jnp.sum(mine, axis=1, keepdims=True).astype(jnp.int32)
    lane_ids = lax.broadcasted_iota(jnp.int32, (groups, width), 1)
    picks_ref[...] = jnp.where(lane_ids == wanted, 1.0, 0.0).astype(jnp.bfloat16)
    sublane = lax.broadcasted_iota(jnp.int32, (block_rows, outputs), 0)
    ends = [jnp.broadcast_to(ends_ref[0:1, window : window + 1], (block_rows, outputs)) for window in range(windows)]
    for peer in range(front):
        first_row = (corner * front + member_of(place, peer, front)) * block_rows
        for window in range(windows):
            masks_ref[peer, window] = jnp.where(sublane + first_row < ends[window], 1.0, 0.0)
    counts = []
    for window in range(windows):
        counts.append(ends[window][0:1].astype(jnp.float32) + (counts[-1] if counts else 0.0))

    def base_sums(window, lines):
        lines = lines + [counts[window]]
        start = 3 * windows * groups + 4 * window
        out_ref[start : start + 4, :] = jnp.concatenate(lines, 0)

    def store(group, window, lines):
        for kind in range(3):
            at = line_at(groups, group, window, kind)
            out_ref[at : at + 1, :] = lines[kind]

    rows = windows * block_rows
    units = range(groups + 2)
    delta, picked = prepare([own_ref], scale_ref[...], picks_ref[...], one_ref, pre_ref)
    fill(units, rows, pre_ref, delta, picked, first_ref)
    result_ref[...] = tail(first_ref, second_ref, two_ref, three_ref)
    tally(
        units, 1, windows, block_rows, lambda peer, window: masks_ref[0, window], result_ref, base_ref, base_sums, store
    )


def late_kernel(front, chunks, *refs):
    pieces = refs[: front - 1]
    (scale_ref, one_ref, two_ref, three_ref, picks_ref, masks_ref, early_ref, out_ref) = refs[front - 1 : front + 7]
    (pre_ref, first_ref, second_ref, result_ref, base_ref) = refs[front + 7 :]
    windows, block_rows = pieces[0].shape[1:3]
    groups = picks_ref.shape[0]
    rows = (front - 1) * windows * block_rows
    stats = 3 * windows * groups
    order = order_of(front)

    def mask_of(peer, window):
        return masks_ref[order[peer], window]

    def base_sums(window, lines):
        at = stats + 4 * window
        out_ref[at : at + 3, :] = early_ref[at : at + 3, :] + jnp.concatenate(lines, 0)
        out_ref[at + 3 : at + 4, :] = early_ref[at + 3 : at + 4, :]

    def store(group, window, lines):
        for kind in range(3):
            at = line_at(groups, group, window, kind)
            out_ref[at : at + 1, :] = early_ref[at : at + 1, :] + lines[kind]

    delta, picked = prepare(list(pieces), scale_ref[...], picks_ref[...], one_ref, pre_ref)
    fill(chunks[0], rows, pre_ref, delta, picked, first_ref.at[0])
    for index, units in enumerate(chunks):
        slot = index % 2
        if index + 1 < len(chunks):
            fill(chunks[index + 1], rows, pre_ref, delta, picked, first_ref.at[1 - slot])
        result_ref[slot] = tail(first_ref.at[slot], second_ref.at[slot], two_ref, three_ref)
        tally(units, front - 1, windows, block_rows, mask_of, result_ref.at[slot], base_ref, base_sums, store)


def conclude_kernel(own_ref, other_ref, out_ref, variance_ref):
    windows, groups = out_ref.shape[1:3]
    stats = 3 * windows * groups
    running = None
    for window in range(windows):
        at = stats + 4 * window
        pieces = [own_ref[at : at + 3] + other_ref[at : at + 3]]
        for kind in range(3):
            line = line_at(groups, 0, window, kind)
            pieces.append(own_ref[line : line + groups] + other_ref[line : line + groups])
        running = pieces if running is None else [former + latter for former, latter in zip(running, pieces)]
        share = 1.0 / own_ref[at + 3 : at + 4]
        base, sum_d, squares_d, cross = running
        mean = base[1:2] * (0.5 * share)
        variance = (base[2:3] - base[1:2] * mean) * (0.5 * share)
        weight = share / variance
        out_ref[0, window] = (cross - (base[0:1] * share) * sum_d) * weight
        out_ref[1, window] = squares_d * (0.5 * weight)
        variance_ref[window : window + 1, :] = variance


def assemble_kernel(front, own_ref, *refs):
    peers = refs[: front - 1]
    settled_ref, first_ref, total_ref, variance_ref = refs[front - 1 :]
    place = lax.rem(lax.axis_index("rows"), front)
    groups = own_ref.shape[2]
    for peer, ref in zip([0, *order_of(front)], [own_ref] + list(peers)):
        start = pl.multiple_of(member_of(place, peer, front) * groups, groups)
        first_ref[:, pl.ds(start, groups), :] = ref[0]
        total_ref[:, pl.ds(start, groups), :] = ref[1]
    variance_ref[...] = settled_ref[...]


def near(values):
    return pltpu.with_memory_space_constraint(values, pltpu.VMEM)


def exchange(values, pairs):
    return lax.ppermute(values, "rows", pairs)


def local(base_a, base_b, input_scale, layer_one, layer_two, layer_three, swap_cols, window_ends):
    windows, block_rows, width = base_a.shape
    size = lax.axis_size("rows")
    total_groups = swap_cols.shape[0]
    hidden = layer_one.shape[1]
    outputs = layer_three.shape[1]
    back = 2 if size % 2 == 0 else 1
    front = size // back
    groups = total_groups // front
    late_rows = (front - 1) * windows * block_rows
    per_chunk = units_per_chunk(groups + 2, late_rows)
    chunks = [range(at, at + per_chunk) for at in range(0, groups + 2, per_chunk)]
    height = (3 * groups + 4) * windows
    order = order_of(front)

    def pairs_of(peer):
        pairs = []
        for device in range(size):
            corner, place = divmod(device, front)
            source = (place ^ peer) if front & (front - 1) == 0 else (place + peer) % front
            pairs.append((corner * front + source, device))
        return pairs

    vmem = pl.BlockSpec(memory_space=pltpu.VMEM)

    def room_of(spaces):
        held = sum(math.prod(space.shape) * jnp.dtype(space.dtype).itemsize for space in spaces)
        return pltpu.CompilerParams(vmem_limit_bytes=held + SPARE_BYTES)

    def work_of(rows):
        return pl.CostEstimate(
            flops=2 * rows * hidden * (hidden + outputs),
            transcendentals=2 * rows * hidden,
            bytes_accessed=2 * (layer_one.size + layer_two.size + layer_three.size),
        )

    own = jnp.stack([base_a, base_b]).astype(jnp.float32)
    own = pl.pallas_call(
        pass_kernel,
        out_shape=pltpu.VMEM(own.shape, own.dtype),
        in_specs=[pl.BlockSpec(memory_space=pltpu.VMEM)],
        out_specs=pl.BlockSpec(memory_space=pltpu.VMEM),
        input_output_aliases={0: 0},
        cost_estimate=pl.CostEstimate(flops=PASS_FLOPS, transcendentals=0, bytes_accessed=0),
        compiler_params=pltpu.CompilerParams(vmem_limit_bytes=1024 * 1024),
        name="pass",
    )(near(own))
    own = near(own)
    received = [exchange(own, pairs_of(peer)) for peer in order]
    scale = input_scale.reshape(1, width)
    scales, one, two, three = near(scale), near(layer_one), near(layer_two), near(layer_three)

    def early(*args):
        return early_kernel(front, *args)

    own_rows = windows * block_rows
    early_rows = (groups + 2) * own_rows
    early_scratch = [
        pltpu.VMEM((2 * own_rows, hidden), jnp.float32),
        pltpu.VMEM((early_rows, hidden), jnp.bfloat16),
        pltpu.VMEM((early_rows, hidden), jnp.bfloat16),
        pltpu.VMEM((early_rows, outputs), jnp.float32),
        pltpu.VMEM((2, own_rows, outputs), jnp.float32),
    ]
    sums, picks, masks = pl.pallas_call(
        early,
        out_shape=(
            pltpu.VMEM((height, outputs), jnp.float32),
            pltpu.VMEM((groups, width), jnp.bfloat16),
            pltpu.VMEM((front, windows, block_rows, outputs), jnp.float32),
        ),
        in_specs=[vmem] * 7,
        out_specs=(vmem,) * 3,
        scratch_shapes=early_scratch,
        cost_estimate=work_of(early_rows),
        compiler_params=room_of(early_scratch),
        name="early",
    )(
        own,
        scales,
        one,
        two,
        three,
        near(swap_cols.reshape(1, total_groups)),
        near(window_ends.reshape(1, windows)),
    )

    def late(*args):
        return late_kernel(front, chunks, *args)

    chunk_rows = per_chunk * late_rows
    late_scratch = [
        pltpu.VMEM((2 * late_rows, hidden), jnp.float32),
        pltpu.VMEM((2, chunk_rows, hidden), jnp.bfloat16),
        pltpu.VMEM((2, chunk_rows, hidden), jnp.bfloat16),
        pltpu.VMEM((2, chunk_rows, outputs), jnp.float32),
        pltpu.VMEM((2, late_rows, outputs), jnp.float32),
    ]
    partial = pl.pallas_call(
        late,
        out_shape=pltpu.VMEM((height, outputs), jnp.float32),
        in_specs=[vmem] * (front + 6),
        out_specs=vmem,
        scratch_shapes=late_scratch,
        cost_estimate=work_of(len(chunks) * chunk_rows),
        compiler_params=room_of(late_scratch),
        name="late",
    )(*(near(value) for value in (*received, scales, one, two, three, picks, masks, sums)))
    partial = near(partial)
    if back == 1:
        other = jnp.zeros_like(partial)
    else:
        other = exchange(partial, [(device, (device + front) % size) for device in range(size)])

    settled, variance = pl.pallas_call(
        conclude_kernel,
        out_shape=(
            pltpu.VMEM((2, windows, groups, outputs), jnp.float32),
            pltpu.VMEM((windows, outputs), jnp.float32),
        ),
        in_specs=[vmem, vmem],
        out_specs=(vmem, vmem),
        compiler_params=pltpu.CompilerParams(vmem_limit_bytes=SPARE_BYTES),
        name="conclude",
    )(partial, near(other))

    gathered = [exchange(settled, pairs_of(peer)) for peer in order]

    def assemble(*args):
        return assemble_kernel(front, *args)

    whole = jax.ShapeDtypeStruct((windows, total_groups, outputs), jnp.float32)
    return pl.pallas_call(
        assemble,
        out_shape=(whole, whole, jax.ShapeDtypeStruct((windows, outputs), jnp.float32)),
        in_specs=[vmem] * (front + 1),
        out_specs=(vmem, vmem, vmem),
        compiler_params=pltpu.CompilerParams(vmem_limit_bytes=SPARE_BYTES),
        name="assemble",
    )(*(near(value) for value in (settled, *gathered, variance)))


def solution(mesh):
    in_specs = (P(None, "rows", None), P(None, "rows", None), P(), P(), P(), P(), P("par"), P())
    out_specs = (P(None, "par", None), P(None, "par", None), P())
    return jax.shard_map(local, mesh=mesh, in_specs=in_specs, out_specs=out_specs, check_vma=False)
```

```python
import math

import jax
import jax.numpy as jnp
from jax import lax
from jax.experimental import pallas as pl
from jax.experimental.pallas import tpu as pltpu
from jax.sharding import PartitionSpec as P

CHUNK_ROWS = 576
COLUMN_TILE = 256
PASS_FLOPS = 4_000_000_000
SPARE_BYTES = 10 * 1024 * 1024


def dot(left, right):
    return jnp.dot(left, right, preferred_element_type=jnp.float32)


def silu_half(half):
    return half + half * jnp.tanh(half)


def units_per_chunk(units, rows):
    return max(count for count in range(1, units + 1) if units % count == 0 and (count == 1 or count * rows <= CHUNK_ROWS))


def order_of(front):
    peers = list(range(1, front))
    return peers[1:2] + peers[:1] + peers[2:]


def member_of(place, peer, front):
    return jnp.bitwise_xor(place, peer) if front & (front - 1) == 0 else lax.rem(place + peer, front)


def total(value):
    return jnp.sum(value, axis=0, keepdims=True)


def prepare(pieces, scale, picks, one_ref, pre_ref):
    windows, block_rows, width = pieces[0].shape[1:]
    hidden = one_ref.shape[1]

    def scaled(which):
        return jnp.concatenate(
            [(piece[which].reshape(windows * block_rows, width) * scale).astype(jnp.bfloat16) for piece in pieces], 0
        )

    inputs_a = scaled(0)
    inputs_b = scaled(1)
    contract = (((1,), (1,)), ((), ()))
    delta = 0.5 * (
        lax.dot_general(inputs_b, picks, contract, preferred_element_type=jnp.float32)
        - lax.dot_general(inputs_a, picks, contract, preferred_element_type=jnp.float32)
    )
    picked = dot(picks, one_ref[...])
    inputs_ab = jnp.concatenate([inputs_a, inputs_b], 0)
    for start in range(0, hidden, COLUMN_TILE):
        tile = slice(start, start + COLUMN_TILE)
        pre_ref[:, tile] = 0.5 * dot(inputs_ab, one_ref[:, tile])
    return delta, picked


def fill(units, rows, pre_ref, delta, picked, filled_ref):
    hidden = pre_ref.shape[1]
    for index, unit in enumerate(units):
        for start in range(0, hidden, COLUMN_TILE):
            tile = slice(start, start + COLUMN_TILE)
            half = pre_ref[rows : 2 * rows, tile] if unit == 1 else pre_ref[:rows, tile]
            if unit >= 2:
                group = unit - 2
                half = half + delta[:, group : group + 1] * picked[group : group + 1, tile]
            filled_ref[index * rows : (index + 1) * rows, tile] = silu_half(half).astype(jnp.bfloat16)


def tail(filled_ref, second_ref, two_ref, three_ref):
    hidden = two_ref.shape[1]
    for start in range(0, hidden, COLUMN_TILE):
        tile = slice(start, start + COLUMN_TILE)
        half = 0.5 * dot(filled_ref[...], two_ref[:, tile])
        second_ref[:, tile] = silu_half(half).astype(jnp.bfloat16)
    return dot(second_ref[...], three_ref[...])


def tally(units, count, windows, block_rows, mask_of, result_ref, base_ref, base_sums, store):
    outputs = result_ref.shape[1]
    rows = count * windows * block_rows
    zero = jnp.zeros((block_rows, outputs), jnp.float32)
    for index, unit in enumerate(units):
        if unit < 2:
            base_ref[unit] = result_ref[index * rows : (index + 1) * rows]
            if unit == 0:
                continue
        for window in range(windows):
            sums = [zero, zero, zero]
            for peer in range(count):
                at = (peer * windows + window) * block_rows
                mask = mask_of(peer, window)
                va = base_ref[0, at : at + block_rows]
                vb = base_ref[1, at : at + block_rows]
                if unit == 1:
                    sums[0] += mask * vb
                    sums[1] += mask * (va + vb)
                    sums[2] += mask * (va * va + vb * vb)
                else:
                    differ = result_ref[index * rows + at : index * rows + at + block_rows] - va
                    masked = mask * differ
                    sums[0] += masked
                    sums[1] += masked * differ
                    sums[2] += masked * vb
            lines = [total(value) for value in sums]
            if unit == 1:
                base_sums(window, lines)
            else:
                store(unit - 2, window, lines)


def line_at(groups, group, window, kind):
    return (window * 3 + kind) * groups + group


def pass_kernel(given_ref, out_ref):
    pass


def early_kernel(
    front, own_ref, scale_ref, one_ref, two_ref, three_ref, cols_ref, ends_ref, out_ref, picks_ref, masks_ref,
    pre_ref, first_ref, second_ref, result_ref, base_ref,
):
    windows, block_rows, width = own_ref.shape[1:]
    groups = picks_ref.shape[0]
    outputs = three_ref.shape[1]
    device = lax.axis_index("rows")
    place = lax.rem(device, front)
    corner = device // front
    total_groups = cols_ref.shape[1]
    line_ids = lax.broadcasted_iota(jnp.int32, (groups, total_groups), 0)
    spot_ids = lax.broadcasted_iota(jnp.int32, (groups, total_groups), 1)
    mine = jnp.where(spot_ids == line_ids + place * groups, cols_ref[...].astype(jnp.float32), 0.0)
    wanted = jnp.sum(mine, axis=1, keepdims=True).astype(jnp.int32)
    lane_ids = lax.broadcasted_iota(jnp.int32, (groups, width), 1)
    picks_ref[...] = jnp.where(lane_ids == wanted, 1.0, 0.0).astype(jnp.bfloat16)
    sublane = lax.broadcasted_iota(jnp.int32, (block_rows, outputs), 0)
    ends = [jnp.broadcast_to(ends_ref[0:1, window : window + 1], (block_rows, outputs)) for window in range(windows)]
    for peer in range(front):
        first_row = (corner * front + member_of(place, peer, front)) * block_rows
        for window in range(windows):
            masks_ref[peer, window] = jnp.where(sublane + first_row < ends[window], 1.0, 0.0)
    counts = []
    for window in range(windows):
        counts.append(ends[window][0:1].astype(jnp.float32) + (counts[-1] if counts else 0.0))

    def base_sums(window, lines):
        lines = lines + [counts[window]]
        start = 3 * windows * groups + 4 * window
        out_ref[start : start + 4, :] = jnp.concatenate(lines, 0)

    def store(group, window, lines):
        for kind in range(3):
            at = line_at(groups, group, window, kind)
            out_ref[at : at + 1, :] = lines[kind]

    rows = windows * block_rows
    units = range(groups + 2)
    delta, picked = prepare([own_ref], scale_ref[...], picks_ref[...], one_ref, pre_ref)
    fill(units, rows, pre_ref, delta, picked, first_ref)
    result_ref[...] = tail(first_ref, second_ref, two_ref, three_ref)
    tally(
        units, 1, windows, block_rows, lambda peer, window: masks_ref[0, window], result_ref, base_ref, base_sums, store
    )


def late_kernel(front, chunks, *refs):
    pieces = refs[: front - 1]
    (scale_ref, one_ref, two_ref, three_ref, picks_ref, masks_ref, early_ref, out_ref) = refs[front - 1 : front + 7]
    (pre_ref, first_ref, second_ref, result_ref, base_ref) = refs[front + 7 :]
    windows, block_rows = pieces[0].shape[1:3]
    groups = picks_ref.shape[0]
    rows = (front - 1) * windows * block_rows
    stats = 3 * windows * groups
    order = order_of(front)

    def mask_of(peer, window):
        return masks_ref[order[peer], window]

    def base_sums(window, lines):
        at = stats + 4 * window
        out_ref[at : at + 3, :] = early_ref[at : at + 3, :] + jnp.concatenate(lines, 0)
        out_ref[at + 3 : at + 4, :] = early_ref[at + 3 : at + 4, :]

    def store(group, window, lines):
        for kind in range(3):
            at = line_at(groups, group, window, kind)
            out_ref[at : at + 1, :] = early_ref[at : at + 1, :] + lines[kind]

    delta, picked = prepare(list(pieces), scale_ref[...], picks_ref[...], one_ref, pre_ref)
    fill(chunks[0], rows, pre_ref, delta, picked, first_ref.at[0])
    for index, units in enumerate(chunks):
        slot = index % 2
        if index + 1 < len(chunks):
            fill(chunks[index + 1], rows, pre_ref, delta, picked, first_ref.at[1 - slot])
        held = pl.ds(0, len(units) * rows)
        result_ref[slot, held] = tail(first_ref.at[slot, held], second_ref.at[slot, held], two_ref, three_ref)
        tally(units, front - 1, windows, block_rows, mask_of, result_ref.at[slot], base_ref, base_sums, store)


def conclude_kernel(own_ref, other_ref, out_ref, variance_ref):
    windows, groups = out_ref.shape[1:3]
    stats = 3 * windows * groups
    running = None
    for window in range(windows):
        at = stats + 4 * window
        pieces = [own_ref[at : at + 3] + other_ref[at : at + 3]]
        for kind in range(3):
            line = line_at(groups, 0, window, kind)
            pieces.append(own_ref[line : line + groups] + other_ref[line : line + groups])
        running = pieces if running is None else [former + latter for former, latter in zip(running, pieces)]
        share = 1.0 / own_ref[at + 3 : at + 4]
        base, sum_d, squares_d, cross = running
        mean = base[1:2] * (0.5 * share)
        variance = (base[2:3] - base[1:2] * mean) * (0.5 * share)
        weight = share / variance
        out_ref[0, window] = (cross - (base[0:1] * share) * sum_d) * weight
        out_ref[1, window] = squares_d * (0.5 * weight)
        variance_ref[window : window + 1, :] = variance


def assemble_kernel(front, own_ref, *refs):
    peers = refs[: front - 1]
    settled_ref, first_ref, total_ref, variance_ref = refs[front - 1 :]
    place = lax.rem(lax.axis_index("rows"), front)
    groups = own_ref.shape[2]
    for peer, ref in zip([0, *order_of(front)], [own_ref] + list(peers)):
        start = pl.multiple_of(member_of(place, peer, front) * groups, groups)
        first_ref[:, pl.ds(start, groups), :] = ref[0]
        total_ref[:, pl.ds(start, groups), :] = ref[1]
    variance_ref[...] = settled_ref[...]


def near(values):
    return pltpu.with_memory_space_constraint(values, pltpu.VMEM)


def exchange(values, pairs):
    return lax.ppermute(values, "rows", pairs)


def local(base_a, base_b, input_scale, layer_one, layer_two, layer_three, swap_cols, window_ends):
    windows, block_rows, width = base_a.shape
    size = lax.axis_size("rows")
    total_groups = swap_cols.shape[0]
    hidden = layer_one.shape[1]
    outputs = layer_three.shape[1]
    back = 2 if size % 2 == 0 else 1
    front = size // back
    groups = total_groups // front
    late_rows = (front - 1) * windows * block_rows
    per_chunk = units_per_chunk(groups + 2, late_rows)
    chunks = [range(at, min(at + per_chunk + 1, groups + 2)) for at in range(0, groups + 2, per_chunk + 1)]
    height = (3 * groups + 4) * windows
    order = order_of(front)

    def pairs_of(peer):
        pairs = []
        for device in range(size):
            corner, place = divmod(device, front)
            source = (place ^ peer) if front & (front - 1) == 0 else (place + peer) % front
            pairs.append((corner * front + source, device))
        return pairs

    vmem = pl.BlockSpec(memory_space=pltpu.VMEM)

    def room_of(spaces):
        held = sum(math.prod(space.shape) * jnp.dtype(space.dtype).itemsize for space in spaces)
        return pltpu.CompilerParams(vmem_limit_bytes=held + SPARE_BYTES)

    def work_of(rows):
        return pl.CostEstimate(
            flops=2 * rows * hidden * (hidden + outputs),
            transcendentals=2 * rows * hidden,
            bytes_accessed=2 * (layer_one.size + layer_two.size + layer_three.size),
        )

    own = jnp.stack([base_a, base_b]).astype(jnp.float32)
    own = pl.pallas_call(
        pass_kernel,
        out_shape=pltpu.VMEM(own.shape, own.dtype),
        in_specs=[pl.BlockSpec(memory_space=pltpu.VMEM)],
        out_specs=pl.BlockSpec(memory_space=pltpu.VMEM),
        input_output_aliases={0: 0},
        cost_estimate=pl.CostEstimate(flops=PASS_FLOPS, transcendentals=0, bytes_accessed=0),
        compiler_params=pltpu.CompilerParams(vmem_limit_bytes=1024 * 1024),
        name="pass",
    )(near(own))
    own = near(own)
    received = [exchange(own, pairs_of(peer)) for peer in order]
    scale = input_scale.reshape(1, width)
    scales, one, two, three = near(scale), near(layer_one), near(layer_two), near(layer_three)

    def early(*args):
        return early_kernel(front, *args)

    own_rows = windows * block_rows
    early_rows = (groups + 2) * own_rows
    early_scratch = [
        pltpu.VMEM((2 * own_rows, hidden), jnp.float32),
        pltpu.VMEM((early_rows, hidden), jnp.bfloat16),
        pltpu.VMEM((early_rows, hidden), jnp.bfloat16),
        pltpu.VMEM((early_rows, outputs), jnp.float32),
        pltpu.VMEM((2, own_rows, outputs), jnp.float32),
    ]
    sums, picks, masks = pl.pallas_call(
        early,
        out_shape=(
            pltpu.VMEM((height, outputs), jnp.float32),
            pltpu.VMEM((groups, width), jnp.bfloat16),
            pltpu.VMEM((front, windows, block_rows, outputs), jnp.float32),
        ),
        in_specs=[vmem] * 7,
        out_specs=(vmem,) * 3,
        scratch_shapes=early_scratch,
        cost_estimate=work_of(early_rows),
        compiler_params=room_of(early_scratch),
        name="early",
    )(
        own,
        scales,
        one,
        two,
        three,
        near(swap_cols.reshape(1, total_groups)),
        near(window_ends.reshape(1, windows)),
    )

    def late(*args):
        return late_kernel(front, chunks, *args)

    chunk_rows = len(chunks[0]) * late_rows
    late_scratch = [
        pltpu.VMEM((2 * late_rows, hidden), jnp.float32),
        pltpu.VMEM((2, chunk_rows, hidden), jnp.bfloat16),
        pltpu.VMEM((2, chunk_rows, hidden), jnp.bfloat16),
        pltpu.VMEM((2, chunk_rows, outputs), jnp.float32),
        pltpu.VMEM((2, late_rows, outputs), jnp.float32),
    ]
    partial = pl.pallas_call(
        late,
        out_shape=pltpu.VMEM((height, outputs), jnp.float32),
        in_specs=[vmem] * (front + 6),
        out_specs=vmem,
        scratch_shapes=late_scratch,
        cost_estimate=work_of(len(chunks) * chunk_rows),
        compiler_params=room_of(late_scratch),
        name="late",
    )(*(near(value) for value in (*received, scales, one, two, three, picks, masks, sums)))
    partial = near(partial)
    if back == 1:
        other = jnp.zeros_like(partial)
    else:
        other = exchange(partial, [(device, (device + front) % size) for device in range(size)])

    settled, variance = pl.pallas_call(
        conclude_kernel,
        out_shape=(
            pltpu.VMEM((2, windows, groups, outputs), jnp.float32),
            pltpu.VMEM((windows, outputs), jnp.float32),
        ),
        in_specs=[vmem, vmem],
        out_specs=(vmem, vmem),
        compiler_params=pltpu.CompilerParams(vmem_limit_bytes=SPARE_BYTES),
        name="conclude",
    )(partial, near(other))

    gathered = [exchange(settled, pairs_of(peer)) for peer in order]

    def assemble(*args):
        return assemble_kernel(front, *args)

    whole = jax.ShapeDtypeStruct((windows, total_groups, outputs), jnp.float32)
    return pl.pallas_call(
        assemble,
        out_shape=(whole, whole, jax.ShapeDtypeStruct((windows, outputs), jnp.float32)),
        in_specs=[vmem] * (front + 1),
        out_specs=(vmem, vmem, vmem),
        compiler_params=pltpu.CompilerParams(vmem_limit_bytes=SPARE_BYTES),
        name="assemble",
    )(*(near(value) for value in (settled, *gathered, variance)))


def solution(mesh):
    in_specs = (P(None, "rows", None), P(None, "rows", None), P(), P(), P(), P(), P("par"), P())
    out_specs = (P(None, "par", None), P(None, "par", None), P())
    return jax.shard_map(local, mesh=mesh, in_specs=in_specs, out_specs=out_specs, check_vma=False)
```
